128 devices in a mesh: row: 8 (over z_lo, x), col: 16 (over y, z_hi, core).
Axes of the slice: x: 4, y: 4, z: 4 (z_hi: 2, z_lo: 2; z = z_hi * 2 + z_lo), core: 2. Of those that a mesh axis runs over, the one named last changes fastest.
Arguments:
- gate_weight: bfloat16 [4608, 36864], P('row', 'col'), may hold values from -8.838835 to 8.838835
- up_weight: bfloat16 [4608, 36864], P('row', 'col'), may hold values from -8.838835 to 8.838835
- routes: int32 [2, 8], replicated, may hold values from 0 to 7, each once within a row
Outputs:
- gate_serving: bfloat16 [4608, 36864], P('col', 'row')
- up_serving: bfloat16 [4608, 36864], P('col', 'row')
- scales: float32 [2, 36864], P(None, 'row')
The draws below stay inside these ranges and needn't reach their ends.
Inputs may be any that keep to these rules, and one draw needn't show every extreme that they name: Each row of routes names every serving rank's piece once.
All inputs are finite; a program needn't handle non-finite values. Where the reference program divides by a largest or mean magnitude, that divisor is 1e-20 or more.
Results may differ from the reference program's by a relative error of at most 0.001.
Values may be sent and summed in bfloat16 or wider, within the bound.
A program may use at most 64 MiB of HBM per device.

```python
import math
import jax
import jax.numpy as jnp

D = 4608
FF = 36864
SERVE_TP = 8
N_ROW = 8
N_COL = 16


def scaled_weight(key, salt):
    base_key = jax.random.fold_in(key, salt)
    first, second, third = jax.random.split(base_key, 3)
    row_scale = jnp.exp(jax.random.uniform(first, (D, 1), jnp.float32, 0.0, math.log(10.0)))
    col_scale = jnp.exp(jax.random.uniform(second, (1, FF), jnp.float32, 0.0, math.log(10.0)))
    noise = jnp.clip(jax.random.normal(third, (D, FF), jnp.float32), -6.0, 6.0)
    values = noise * row_scale * col_scale / math.sqrt(D)
    return values.astype(jnp.bfloat16)


def draw_gate_weight(key, part):
    return scaled_weight(key, 11)


def draw_up_weight(key, part):
    return scaled_weight(key, 23)


def setup_inputs(seed: int = 0) -> dict:
    keys = jax.random.split(jax.random.key(seed), 4)
    return {
        "gate_weight": draw_gate_weight(jax.random.fold_in(keys[3], 71), 0),
        "up_weight": draw_up_weight(jax.random.fold_in(keys[3], 71), 0),
        "routes": jax.vmap(lambda own: jax.random.permutation(own, SERVE_TP))(jax.random.split(keys[2], 2)).reshape((2, SERVE_TP)).astype(jnp.int32),
    }


EPSILON = 1e-6
LIMIT = 4.0


def convert(weight, order):
    block_len = FF // (N_ROW * N_COL)
    peaks = jnp.max(jnp.abs(weight), axis=0).astype(jnp.float32)
    factor = LIMIT / (peaks + EPSILON)
    quant = (weight.astype(jnp.float32) * factor[None, :]).astype(jnp.bfloat16)
    shaped = quant.reshape(D, N_COL, N_ROW, block_len)
    chosen = jnp.take(shaped, order, axis=2).transpose(0, 2, 1, 3).reshape(D, FF)
    scale_table = ((peaks + EPSILON) / LIMIT).reshape(N_COL, N_ROW, block_len)
    scale_line = jnp.take(scale_table, order, axis=1).transpose(1, 0, 2).reshape(FF)
    return chosen, scale_line


def reference(gate_weight, up_weight, routes):
    gate_serving, gate_scale = convert(gate_weight, routes[0])
    up_serving, up_scale = convert(up_weight, routes[1])
    return gate_serving, up_serving, jnp.stack([gate_scale, up_scale])
```

```python
import functools

import jax
import jax.numpy as jnp
from jax import lax
from jax.experimental import pallas as pl
from jax.experimental.pallas import tpu as pltpu
from jax.sharding import PartitionSpec as P

MESH = pl.DeviceIdType.MESH
EPSILON = 1e-06
LIMIT = 4.0
SIDE = 288
PART = 96
PARTS = SIDE // PART
TAIL = PART // 4
ROWS = 2 * PART + TAIL
CHUNKS = 2 * PARTS


def lanes(rows):
    return lax.broadcasted_iota(jnp.int32, (rows, 128), 1)


def pack_kernel(routes, gate_ref, up_ref, out_ref, peak_ref):
    step = pl.program_id(0)

    @pl.when(step == 0)
    def _():
        peak_ref[...] = jnp.zeros_like(peak_ref)

    lane, lane_tail = lanes(PART), lanes(TAIL)
    for proj, ref in enumerate((gate_ref, up_ref)):
        for rank in range(8):
            piece = routes[proj, rank]
            start = pl.multiple_of(((9 * piece) // 4) * 128, 128)
            shift = 32 * lax.rem(piece, 4)
            back = lax.rem(128 - shift, 128)
            tiles = [
                pltpu.roll(ref[:, pl.ds(start + 128 * t, 128)].astype(jnp.float32), back, 1)
                for t in range(3)
            ]
            keep = lane < 128 - shift
            full = [jnp.where(keep, tiles[0], tiles[1]), jnp.where(keep, tiles[1], tiles[2])]
            tail = tiles[2][:TAIL]
            for g in range(1, 4):
                moved = pltpu.roll(tiles[2][g * TAIL : (g + 1) * TAIL], 32 * g, 1)
                tail = jnp.where(lane_tail < 32 * g, tail, moved)
            out_ref[rank, 0, proj, 0, :PART] = full[0].astype(jnp.bfloat16)
            out_ref[rank, 0, proj, 0, PART : 2 * PART] = full[1].astype(jnp.bfloat16)
            out_ref[rank, 0, proj, 0, 2 * PART :] = tail.astype(jnp.bfloat16)
            for t, value in enumerate((*full, tiles[2])):
                row = 3 * proj + t
                peak_ref[rank, row : row + 1] = jnp.maximum(
                    peak_ref[rank, row : row + 1],
                    jnp.max(jnp.abs(value), axis=0, keepdims=True),
                )


def pack(gate, up, routes):
    return pl.pallas_call(
        pack_kernel,
        out_shape=(
            jax.ShapeDtypeStruct((8, 2, 2, PARTS, ROWS, 128), jnp.bfloat16),
            jax.ShapeDtypeStruct((8, 8, 128), jnp.float32),
        ),
        grid_spec=pltpu.PrefetchScalarGridSpec(
            num_scalar_prefetch=1,
            grid=(2 * PARTS,),
            in_specs=[pl.BlockSpec((PART, 2304), lambda i, _: (i, 0))] * 2,
            out_specs=(
                pl.BlockSpec(
                    (8, 1, 2, 1, ROWS, 128),
                    lambda i, _: (0, i // PARTS, 0, lax.rem(i, PARTS), 0, 0),
                ),
                pl.BlockSpec((8, 8, 128), lambda i, _: (0, 0, 0)),
            ),
        ),
        compiler_params=pltpu.CompilerParams(vmem_limit_bytes=24 * 2**20),
    )(routes, gate, up)


def place():
    r, c = lax.axis_index("row"), lax.axis_index("col")
    return r % 4, c // 4, (c // 2 % 2) * 2 + r // 4, c % 2


def device(x, y, z, k):
    return ((z % 2) * 4 + x, y * 4 + (z // 2) * 2 + k)


def remote(src, dst, send, recv, to):
    return pltpu.make_async_remote_copy(
        src_ref=src, dst_ref=dst, send_sem=send, recv_sem=recv, device_id=to, device_id_type=MESH
    )


def wait_bytes(ref, sem):
    pltpu.make_async_copy(ref, ref, sem).wait()


def move_kernel(
    src, peaks, out, every, relay, mine, total, gathered, sends, relay_sems, out_sem, peak_sems
):
    x, y, z, k = place()
    z_lo, z_hi = z % 2, z // 2
    row, col = lax.axis_index("row"), lax.axis_index("col")
    goal = 2 * z_lo + x // 2
    stay = goal == y
    near = x % 2 == z_hi
    slot = goal * 4 + z_hi * 2 + k
    own = 2 * (z_lo * 4 + x) + k

    barrier = pltpu.get_barrier_semaphore()
    for n in range(1, 32):
        other = device((x + n // 8) % 4, y, (z + n // 2 % 4) % 4, (k + n % 2) % 2)
        pl.semaphore_signal(barrier, 1, device_id=other, device_id_type=MESH)
    for n in range(12):
        other = device(x, (y + 1 + n // 4) % 4, (z + 2 * (n // 2 % 2)) % 4, (k + n % 2) % 2)
        pl.semaphore_signal(barrier, 1, device_id=other, device_id_type=MESH)
    pl.semaphore_wait(barrier, 43)

    def first(dx, zl, h, p):
        xd, zd = (x + dx) % 4, 2 * (x % 2) + zl
        block = src.at[2 * (zl * 4 + xd) + h, p]
        to = device(xd, y, zd, h)
        go = jnp.logical_not(jnp.logical_and(zd == z, h == k)) if dx == 0 else None

        def both():
            @pl.when(stay)
            def _():
                remote(block, out.at[col, p], sends.at[0], out_sem, to).start()

            @pl.when(jnp.logical_not(stay))
            def _():
                remote(block, relay.at[slot, p], sends.at[0], relay_sems.at[slot, p], to).start()

        if go is None:
            both()
        else:
            pl.when(go)(both)

    def second(dy, q, p):
        yd = (y + dy) % 4
        here = yd * 4 + q
        to = device(x, yd, z, k)
        target = out.at[y * 4 + q, p]
        local = jnp.logical_and(near, jnp.logical_and(yd == goal, q == z_hi * 2 + k))

        @pl.when(local)
        def _():
            remote(src.at[own, p], target, sends.at[1], out_sem, to).start()

        @pl.when(jnp.logical_not(local))
        def _():
            wait_bytes(relay.at[here, p], relay_sems.at[here, p])
            remote(relay.at[here, p], target, sends.at[1], out_sem, to).start()

    firsts = [(dx, zl, h) for h in range(2) for zl in range(2) for dx in (2, 1, 3, 0)]
    seconds = [(dy, q) for dy in (2, 1, 3) for q in range(4)]

    def open_round(p, _):
        for f in firsts:
            first(*f, p)
        return 0

    def full_round(p, _):
        for i, f in enumerate(firsts):
            if i < len(seconds):
                second(*seconds[i], p)
            first(*f, p + 2)
        return 0

    def last_round(p, _):
        for s in seconds:
            second(*s, p)
        return 0

    lax.fori_loop(0, 1, open_round, 0)

    mine[row] = peaks[row]
    for n in range(1, 8):
        xd, zl = (x + n % 4) % 4, (z_lo + n // 4) % 2
        rank = zl * 4 + xd
        remote(
            peaks.at[rank], mine.at[row], sends.at[2], peak_sems.at[0], device(xd, y, 2 * z_hi + zl, k)
        ).start()

    keep = jnp.logical_and(near, stay)

    @pl.when(keep)
    def _():
        out[col] = src[own]

    lax.fori_loop(1, 2, open_round, 0)
    wait_bytes(mine.at[pl.ds(0, 7)], peak_sems.at[0])
    total[...] = jnp.max(mine[...], axis=0)
    lax.fori_loop(0, 1, full_round, 0)
    gathered[col] = total[...]
    for n in range(1, 16):
        yd, zd, kd = (y + n // 4) % 4, (z + 2 * (n // 2 % 2)) % 4, (k + n % 2) % 2
        remote(total, gathered.at[col], sends.at[3], peak_sems.at[1], device(x, yd, zd, kd)).start()
    lax.fori_loop(1, CHUNKS - 2, full_round, 0)
    lax.fori_loop(CHUNKS - 2, CHUNKS, last_round, 0)
    wait_bytes(gathered.at[pl.ds(0, 15)], peak_sems.at[1])
    every[...] = gathered[...]

    @pl.when(keep)
    def _():
        wait_bytes(out.at[pl.ds(0, 15)], out_sem)

    @pl.when(jnp.logical_not(keep))
    def _():
        wait_bytes(out, out_sem)

    @pl.when(near)
    def _():
        wait_bytes(src.at[pl.ds(0, 15)], sends.at[0])

    @pl.when(jnp.logical_not(near))
    def _():
        wait_bytes(src, sends.at[0])

    wait_bytes(src.at[pl.ds(0, 12)], sends.at[1])
    wait_bytes(mine.at[pl.ds(0, 7)], sends.at[2])
    wait_bytes(gathered.at[pl.ds(0, 15)], sends.at[3])


def move(blocks, peaks):
    shape = (16, CHUNKS, ROWS, 128)
    return pl.pallas_call(
        move_kernel,
        out_shape=(
            jax.ShapeDtypeStruct(shape, jnp.bfloat16),
            jax.ShapeDtypeStruct((16, 8, 128), jnp.float32),
        ),
        in_specs=[pl.BlockSpec(memory_space=pltpu.VMEM)] * 2,
        out_specs=(pl.BlockSpec(memory_space=pltpu.VMEM),) * 2,
        scratch_shapes=[
            pltpu.VMEM(shape, jnp.bfloat16),
            pltpu.VMEM((8, 8, 128), jnp.float32),
            pltpu.VMEM((8, 128), jnp.float32),
            pltpu.VMEM((16, 8, 128), jnp.float32),
            pltpu.SemaphoreType.DMA((4,)),
            pltpu.SemaphoreType.DMA((16, CHUNKS)),
            pltpu.SemaphoreType.DMA,
            pltpu.SemaphoreType.DMA((2,)),
        ],
        compiler_params=pltpu.CompilerParams(
            collective_id=0, has_side_effects=True, vmem_limit_bytes=24 * 2**20
        ),
    )(blocks.reshape(shape), peaks)


def joined(pieces, rows):
    lane = lanes(rows)
    tiles = []
    spill = None
    for i, (a, b, tail) in enumerate(pieces):
        if i:
            a, b = pltpu.roll(a, 32 * i, 1), pltpu.roll(b, 32 * i, 1)
            tiles.append(jnp.where(lane < 32 * i, spill, a))
            tiles.append(jnp.where(lane < 32 * i, a, b))
            spill = jnp.where(lane < 32 * i, b, tail)
        else:
            tiles += [a, b]
            spill = tail
    tiles.append(spill)
    return tiles


def finish_kernel(blocks, peaks, gate_ref, up_ref, scale_ref, factor):
    @pl.when(pl.program_id(0) == 0)
    def _():
        for proj in range(2):
            for quad in range(4):
                pieces = []
                for i in range(4):
                    value = peaks[4 * quad + i]
                    a, b, t = (value[3 * proj + n : 3 * proj + n + 1] for n in range(3))
                    pieces.append((a, b, pltpu.roll(t, 32 * i, 1) if i else t))
                for n, tile in enumerate(joined(pieces, 1)):
                    at = pl.ds(128 * (9 * quad + n), 128)
                    scale_ref[proj : proj + 1, at] = (tile + EPSILON) / LIMIT
                    factor[proj : proj + 1, at] = LIMIT / (tile + EPSILON)

    for proj, ref in enumerate((gate_ref, up_ref)):
        for quad in range(4):
            pieces = []
            for i in range(4):
                value = blocks[4 * quad + i, proj, 0].astype(jnp.float32)
                last = value[2 * PART :]
                tail = jnp.concatenate(
                    [pltpu.roll(last, (32 * (i - g)) % 128, 1) if i != g else last for g in range(4)],
                    axis=0,
                )
                pieces.append((value[:PART], value[PART : 2 * PART], tail))
            for n, tile in enumerate(joined(pieces, PART)):
                at = pl.ds(128 * (9 * quad + n), 128)
                ref[:, at] = (tile * factor[proj : proj + 1, at]).astype(jnp.bfloat16)


def finish(blocks, peaks):
    return pl.pallas_call(
        finish_kernel,
        out_shape=(
            jax.ShapeDtypeStruct((SIDE, 4608), jnp.bfloat16),
            jax.ShapeDtypeStruct((SIDE, 4608), jnp.bfloat16),
            jax.ShapeDtypeStruct((2, 4608), jnp.float32),
        ),
        grid=(PARTS,),
        in_specs=[
            pl.BlockSpec((16, 2, 1, ROWS, 128), lambda j: (0, 0, j, 0, 0)),
            pl.BlockSpec((16, 8, 128), lambda j: (0, 0, 0)),
        ],
        out_specs=(
            pl.BlockSpec((PART, 4608), lambda j: (j, 0)),
            pl.BlockSpec((PART, 4608), lambda j: (j, 0)),
            pl.BlockSpec((2, 4608), lambda j: (0, 0)),
        ),
        scratch_shapes=[pltpu.VMEM((2, 4608), jnp.float32)],
        compiler_params=pltpu.CompilerParams(vmem_limit_bytes=24 * 2**20),
    )(blocks.reshape(16, 2, PARTS, ROWS, 128), peaks)


def shards(gate_weight, up_weight, routes):
    return finish(*move(*pack(gate_weight, up_weight, routes)))


def solution(mesh):
    return jax.shard_map(
        shards,
        mesh=mesh,
        in_specs=(P("row", "col"), P("row", "col"), P()),
        out_specs=(P("col", "row"), P("col", "row"), P(None, "row")),
        check_vma=False,
    )
```

```python
import functools

import jax
import jax.numpy as jnp
from jax import lax
from jax.experimental import pallas as pl
from jax.experimental.pallas import tpu as pltpu
from jax.sharding import PartitionSpec as P

MESH = pl.DeviceIdType.MESH
EPSILON = 1e-06
LIMIT = 4.0
SIDE = 288
PART = 96
PARTS = SIDE // PART
TAIL = PART // 4
ROWS = 2 * PART + TAIL
CHUNKS = 2 * PARTS


def lanes(rows):
    return lax.broadcasted_iota(jnp.int32, (rows, 128), 1)


def place():
    r, c = lax.axis_index("row"), lax.axis_index("col")
    return r % 4, c // 4, (c // 2 % 2) * 2 + r // 4, c % 2


def device(x, y, z, k):
    return ((z % 2) * 4 + x, y * 4 + (z // 2) * 2 + k)


def remote(src, dst, send, recv, to):
    return pltpu.make_async_remote_copy(
        src_ref=src, dst_ref=dst, send_sem=send, recv_sem=recv, device_id=to, device_id_type=MESH
    )


def wait_bytes(ref, sem):
    pltpu.make_async_copy(ref, ref, sem).wait()


def aligned(ref, lead, piece):
    start, shift = 9 * piece // 4 * 128, 32 * (piece % 4)
    a, b, c = (
        ref[(*lead, slice(start + 128 * t, start + 128 * (t + 1)))].astype(jnp.float32) for t in range(3)
    )
    if not shift:
        return a, b, c
    a, b, c = (pltpu.roll(value, 128 - shift, 1) for value in (a, b, c))
    keep = lanes(a.shape[0]) < 128 - shift
    return jnp.where(keep, a, b), jnp.where(keep, b, c), c


def pack(routes, slab, packed, src, p):
    lane_tail = lanes(TAIL)
    for piece in range(8):
        for h in range(2):
            a, b, c = aligned(slab, (2 * p + h, slice(None)), piece)
            last = c[:TAIL]
            for g in range(1, 4):
                moved = pltpu.roll(c[g * TAIL : (g + 1) * TAIL], 32 * g, 1)
                last = jnp.where(lane_tail < 32 * g, last, moved)
            packed[2 * piece + h, :PART] = a.astype(jnp.bfloat16)
            packed[2 * piece + h, PART : 2 * PART] = b.astype(jnp.bfloat16)
            packed[2 * piece + h, 2 * PART :] = last.astype(jnp.bfloat16)
    for rank in range(8):
        piece = routes[p // PARTS, rank]
        for h in range(2):
            src[2 * rank + h, p] = packed[2 * piece + h]


def local_peaks(routes, slab, line, pieces, peaks):
    for proj in range(2):
        for at in range(0, 2304, 256):
            top = jnp.abs(slab[2 * PARTS * proj, :, at : at + 256])
            for n in range(1, 2 * PARTS):
                top = jnp.maximum(top, jnp.abs(slab[2 * PARTS * proj + n, :, at : at + 256]))
            line[proj : proj + 1, at : at + 256] = jnp.max(top.astype(jnp.float32), axis=0, keepdims=True)
    for proj in range(2):
        for piece in range(8):
            rows = aligned(line, (slice(proj, proj + 1),), piece)
            for t in range(3):
                pieces[8 * proj + piece, 3 * proj + t : 3 * proj + t + 1] = rows[t]
    upper = lax.broadcasted_iota(jnp.int32, (8, 128), 0) < 3
    for rank in range(8):
        peaks[rank] = jnp.where(upper, pieces[routes[0, rank]], pieces[8 + routes[1, rank]])


def joined(pieces, rows):
    lane = lanes(rows)
    tiles = []
    spill = None
    for i, (a, b, tail) in enumerate(pieces):
        if i:
            a, b = pltpu.roll(a, 32 * i, 1), pltpu.roll(b, 32 * i, 1)
            tiles.append(jnp.where(lane < 32 * i, spill, a))
            tiles.append(jnp.where(lane < 32 * i, a, b))
            spill = jnp.where(lane < 32 * i, b, tail)
        else:
            tiles += [a, b]
            spill = tail
    tiles.append(spill)
    return tiles


def factors(gathered, scales, factor):
    for proj in range(2):
        for quad in range(4):
            pieces = []
            for i in range(4):
                value = gathered[4 * quad + i]
                a, b, t = (value[3 * proj + n : 3 * proj + n + 1] for n in range(3))
                pieces.append((a, b, pltpu.roll(t, 32 * i, 1) if i else t))
            for n, tile in enumerate(joined(pieces, 1)):
                at = pl.ds(128 * (9 * quad + n), 128)
                scales[proj : proj + 1, at] = (tile + EPSILON) / LIMIT
                factor[proj, :, at] = LIMIT / (tile + EPSILON)


def lay_out(blocks, factor, out, p):
    proj = p // PARTS
    rows = pl.ds(pl.multiple_of((p % PARTS) * PART, PART), PART)
    for quad in range(4):
        pieces = []
        for i in range(4):
            value = blocks[4 * quad + i, p].astype(jnp.float32)
            last = value[2 * PART :]
            tail = jnp.concatenate(
                [pltpu.roll(last, (32 * (i - g)) % 128, 1) if i != g else last for g in range(4)],
                axis=0,
            )
            pieces.append((value[:PART], value[PART : 2 * PART], tail))
        for n, tile in enumerate(joined(pieces, PART)):
            at = pl.ds(128 * (9 * quad + n), 128)
            out[proj, rows, at] = (tile * factor[proj, :, at]).astype(jnp.bfloat16)


def move_kernel(
    routes, gate, up, gate_out, up_out, scales, slab, src, relay, out, final, packed, line, pieces, peaks, mine, total, gathered, factor,
    slab_sems, sends, relay_sems, out_sems, peak_sems, final_sems
):
    x, y, z, k = place()
    z_lo, z_hi = z % 2, z // 2
    row, col = lax.axis_index("row"), lax.axis_index("col")
    goal = 2 * z_lo + x // 2
    stay = goal == y
    near = x % 2 == z_hi
    slot = goal * 4 + z_hi * 2 + k
    own = 2 * (z_lo * 4 + x) + k
    keep = jnp.logical_and(near, stay)

    def slab_copy(ref, p, h):
        rows = pl.ds(h * SIDE + (p % PARTS) * PART, PART)
        return pltpu.make_async_copy(ref.at[rows], slab.at[2 * p + h], slab_sems.at[2 * p + h])

    for p in range(CHUNKS):
        for h in range(2):
            slab_copy((gate, up)[p // PARTS], p, h).start()

    barrier = pltpu.get_barrier_semaphore()
    for n in range(1, 32):
        other = device((x + n // 8) % 4, y, (z + n // 2 % 4) % 4, (k + n % 2) % 2)
        pl.semaphore_signal(barrier, 1, device_id=other, device_id_type=MESH)
    for n in range(12):
        other = device(x, (y + 1 + n // 4) % 4, (z + 2 * (n // 2 % 2)) % 4, (k + n % 2) % 2)
        pl.semaphore_signal(barrier, 1, device_id=other, device_id_type=MESH)

    def first(hi, zi, dx, p):
        h, zl = (k + hi) % 2, (z_lo + zi) % 2
        xd, zd = (x + dx) % 4, 2 * (x % 2) + zl
        block = src.at[2 * (zl * 4 + xd) + h, p]
        to = device(xd, y, zd, h)
        at_all = jnp.logical_not(near) if (hi, zi, dx) == (0, 0, 0) else True

        @pl.when(jnp.logical_and(at_all, stay))
        def _():
            remote(block, out.at[col, p], sends.at[0], out_sems.at[p], to).start()

        @pl.when(jnp.logical_and(at_all, jnp.logical_not(stay)))
        def _():
            remote(block, relay.at[slot, p], sends.at[0], relay_sems.at[slot, p], to).start()

    def second(hi, zi, a, zs, p):
        zl, ks = (z_lo + zi) % 2, (k + hi) % 2
        yd = 2 * zl + a
        q = zs * 2 + ks
        here = yd * 4 + q
        to = device(x, yd, z, k)
        target = out.at[y * 4 + q, p]
        go = yd != y
        if (hi, zi) == (0, 0):
            local = jnp.logical_and(near, jnp.logical_and(yd == goal, zs == z_hi))

            @pl.when(jnp.logical_and(go, local))
            def _():
                remote(src.at[own, p], target, sends.at[1], out_sems.at[p], to).start()

            go = jnp.logical_and(go, jnp.logical_not(local))

        @pl.when(go)
        def _():
            wait_bytes(relay.at[here, p], relay_sems.at[here, p])
            remote(relay.at[here, p], target, sends.at[1], out_sems.at[p], to).start()

    groups = [(0, 0), (0, 1), (1, 0), (1, 1)]
    firsts = [(*g, dx) for g in groups for dx in (1, 3, 2, 0)]
    seconds = [(*g, a, zs) for g in groups for a in range(2) for zs in range(2)]

    def prepare(p):
        pack(routes, slab, packed, src, p)

        @pl.when(keep)
        def _():
            out[col, p] = src[own, p]

    def full_round(p, _):
        prepare(p + 2)
        for f, s in zip(firsts, seconds):
            second(*s, p)
            first(*f, p + 2)
        return 0

    def last_round(p, _):
        for s in seconds:
            second(*s, p)
        return 0

    def result(proj, p):
        rows = pl.ds(pl.multiple_of((p % PARTS) * PART, PART), PART)
        return pltpu.make_async_copy(final.at[proj, rows], (gate_out, up_out)[proj].at[rows], final_sems.at[p])

    def arrived(p, _):
        @pl.when(keep)
        def _():
            wait_bytes(out.at[pl.ds(0, 15), p], out_sems.at[p])

        @pl.when(jnp.logical_not(keep))
        def _():
            wait_bytes(out.at[:, p], out_sems.at[p])

        lay_out(out, factor, final, p)
        for proj in range(2):
            pl.when(p // PARTS == proj)(result(proj, p).start)
        return 0

    for h in range(2):
        slab_copy(gate, 0, h).wait()
    prepare(0)
    pl.semaphore_wait(barrier, 43)
    for f in firsts:
        first(*f, 0)

    for n in range(2, 2 * CHUNKS):
        slab_copy(gate, n // 2, n % 2).wait()
    local_peaks(routes, slab, line, pieces, peaks)
    mine[row] = peaks[row]
    for n in range(1, 8):
        xd, zl = (x + n % 4) % 4, (z_lo + n // 4) % 2
        to = device(xd, y, 2 * z_hi + zl, k)
        remote(peaks.at[zl * 4 + xd], mine.at[row], sends.at[2], peak_sems.at[0], to).start()

    prepare(1)
    for f in firsts:
        first(*f, 1)
    lax.fori_loop(0, 1, full_round, 0)
    wait_bytes(mine.at[pl.ds(0, 7)], peak_sems.at[0])
    total[...] = jnp.max(mine[...], axis=0)
    gathered[col] = total[...]
    lax.fori_loop(1, 2, full_round, 0)
    for n in range(1, 4):
        to = device(x, y, (z + 2 * (n // 2)) % 4, (k + n % 2) % 2)
        remote(total, gathered.at[col], sends.at[3], peak_sems.at[1], to).start()
    lax.fori_loop(2, 3, full_round, 0)
    lax.fori_loop(3, 4, full_round, 0)
    wait_bytes(gathered.at[pl.ds(0, 3)], peak_sems.at[1])
    four = pl.ds(4 * y, 4)
    for dy in range(1, 4):
        to = device(x, (y + dy) % 4, z, k)
        remote(gathered.at[four], gathered.at[four], sends.at[4], peak_sems.at[2], to).start()
    lax.fori_loop(CHUNKS - 2, CHUNKS - 1, last_round, 0)
    lax.fori_loop(CHUNKS - 1, CHUNKS, last_round, 0)
    wait_bytes(gathered.at[pl.ds(0, 12)], peak_sems.at[2])
    factors(gathered, scales, factor)
    lax.fori_loop(0, CHUNKS, arrived, 0)

    @pl.when(near)
    def _():
        wait_bytes(src.at[pl.ds(0, 15)], sends.at[0])

    @pl.when(jnp.logical_not(near))
    def _():
        wait_bytes(src, sends.at[0])

    wait_bytes(src.at[pl.ds(0, 12)], sends.at[1])
    wait_bytes(mine.at[pl.ds(0, 7)], sends.at[2])
    wait_bytes(gathered.at[pl.ds(0, 3)], sends.at[3])
    wait_bytes(gathered.at[pl.ds(0, 12)], sends.at[4])
    for p in range(CHUNKS):
        result(p // PARTS, p).wait()


def move(gate, up, routes):
    shape = (16, CHUNKS, ROWS, 128)
    return pl.pallas_call(
        move_kernel,
        out_shape=(
            jax.ShapeDtypeStruct((SIDE, 4608), jnp.bfloat16),
            jax.ShapeDtypeStruct((SIDE, 4608), jnp.bfloat16),
            jax.ShapeDtypeStruct((2, 4608), jnp.float32),
        ),
        in_specs=[
            pl.BlockSpec(memory_space=pltpu.SMEM),
            pl.BlockSpec(memory_space=pltpu.HBM),
            pl.BlockSpec(memory_space=pltpu.HBM),
        ],
        out_specs=(
            pl.BlockSpec(memory_space=pltpu.HBM),
            pl.BlockSpec(memory_space=pltpu.HBM),
            pl.BlockSpec(memory_space=pltpu.VMEM),
        ),
        scratch_shapes=[
            pltpu.VMEM((2 * CHUNKS, PART, 2304), jnp.bfloat16),
            pltpu.VMEM(shape, jnp.bfloat16),
            pltpu.VMEM(shape, jnp.bfloat16),
            pltpu.VMEM(shape, jnp.bfloat16),
            pltpu.VMEM((2, SIDE, 4608), jnp.bfloat16),
            pltpu.VMEM((16, ROWS, 128), jnp.bfloat16),
            pltpu.VMEM((2, 2304), jnp.float32),
            pltpu.VMEM((16, 8, 128), jnp.float32),
            pltpu.VMEM((8, 8, 128), jnp.float32),
            pltpu.VMEM((8, 8, 128), jnp.float32),
            pltpu.VMEM((8, 128), jnp.float32),
            pltpu.VMEM((16, 8, 128), jnp.float32),
            pltpu.VMEM((2, 1, 4608), jnp.float32),
            pltpu.SemaphoreType.DMA((2 * CHUNKS,)),
            pltpu.SemaphoreType.DMA((5,)),
            pltpu.SemaphoreType.DMA((16, CHUNKS)),
            pltpu.SemaphoreType.DMA((CHUNKS,)),
            pltpu.SemaphoreType.DMA((3,)),
            pltpu.SemaphoreType.DMA((CHUNKS,)),
        ],
        compiler_params=pltpu.CompilerParams(
            collective_id=0, has_side_effects=True, vmem_limit_bytes=60 * 2**20
        ),
    )(routes, gate, up)


def shards(gate_weight, up_weight, routes):
    return move(gate_weight, up_weight, routes)


def solution(mesh):
    return jax.shard_map(
        shards,
        mesh=mesh,
        in_specs=(P("row", "col"), P("row", "col"), P()),
        out_specs=(P("col", "row"), P("col", "row"), P(None, "row")),
        check_vma=False,
    )
```

```python
import functools

import jax
import jax.numpy as jnp
from jax import lax
from jax.experimental import pallas as pl
from jax.experimental.pallas import tpu as pltpu
from jax.sharding import PartitionSpec as P

MESH = pl.DeviceIdType.MESH
EPSILON = 1e-06
LIMIT = 4.0
SIDE = 288
PART = 96
PARTS = SIDE // PART
TAIL = PART // 4
ROWS = 2 * PART + TAIL
CHUNKS = 2 * PARTS


def lanes(rows):
    return lax.broadcasted_iota(jnp.int32, (rows, 128), 1)


def place():
    r, c = lax.axis_index("row"), lax.axis_index("col")
    return r % 4, c // 4, (c // 2 % 2) * 2 + r // 4, c % 2


def device(x, y, z, k):
    return ((z % 2) * 4 + x, y * 4 + (z // 2) * 2 + k)


def remote(src, dst, send, recv, to):
    return pltpu.make_async_remote_copy(
        src_ref=src, dst_ref=dst, send_sem=send, recv_sem=recv, device_id=to, device_id_type=MESH
    )


def wait_bytes(ref, sem):
    pltpu.make_async_copy(ref, ref, sem).wait()


def aligned(ref, lead, piece):
    start, shift = 9 * piece // 4 * 128, 32 * (piece % 4)
    a, b, c = (
        ref[(*lead, slice(start + 128 * t, start + 128 * (t + 1)))].astype(jnp.float32) for t in range(3)
    )
    if not shift:
        return a, b, c
    a, b, c = (pltpu.roll(value, 128 - shift, 1) for value in (a, b, c))
    keep = lanes(a.shape[0]) < 128 - shift
    return jnp.where(keep, a, b), jnp.where(keep, b, c), c


def pack(routes, slab, packed, src, p, halves):
    lane_tail = lanes(TAIL)
    for piece in range(8):
        for h in halves:
            a, b, c = aligned(slab, (2 * p + h, slice(None)), piece)
            last = c[:TAIL]
            for g in range(1, 4):
                moved = pltpu.roll(c[g * TAIL : (g + 1) * TAIL], 32 * g, 1)
                last = jnp.where(lane_tail < 32 * g, last, moved)
            packed[2 * piece + h, :PART] = a.astype(jnp.bfloat16)
            packed[2 * piece + h, PART : 2 * PART] = b.astype(jnp.bfloat16)
            packed[2 * piece + h, 2 * PART :] = last.astype(jnp.bfloat16)
    for rank in range(8):
        piece = routes[p // PARTS, rank]
        for h in halves:
            src[2 * rank + h, p] = packed[2 * piece + h]


def local_peaks(routes, slab, line, pieces, peaks):
    for proj in range(2):
        for at in range(0, 2304, 256):
            top = jnp.abs(slab[2 * PARTS * proj, :, at : at + 256])
            for n in range(1, 2 * PARTS):
                top = jnp.maximum(top, jnp.abs(slab[2 * PARTS * proj + n, :, at : at + 256]))
            line[proj : proj + 1, at : at + 256] = jnp.max(top.astype(jnp.float32), axis=0, keepdims=True)
    for proj in range(2):
        for piece in range(8):
            rows = aligned(line, (slice(proj, proj + 1),), piece)
            for t in range(3):
                pieces[8 * proj + piece, 3 * proj + t : 3 * proj + t + 1] = rows[t]
    upper = lax.broadcasted_iota(jnp.int32, (8, 128), 0) < 3
    for rank in range(8):
        peaks[rank] = jnp.where(upper, pieces[routes[0, rank]], pieces[8 + routes[1, rank]])


def joined(pieces, rows):
    lane = lanes(rows)
    tiles = []
    spill = None
    for i, (a, b, tail) in enumerate(pieces):
        if i:
            a, b = pltpu.roll(a, 32 * i, 1), pltpu.roll(b, 32 * i, 1)
            tiles.append(jnp.where(lane < 32 * i, spill, a))
            tiles.append(jnp.where(lane < 32 * i, a, b))
            spill = jnp.where(lane < 32 * i, b, tail)
        else:
            tiles += [a, b]
            spill = tail
    tiles.append(spill)
    return tiles


def factors(gathered, scales, factor):
    for proj in range(2):
        for quad in range(4):
            pieces = []
            for i in range(4):
                value = gathered[4 * quad + i]
                a, b, t = (value[3 * proj + n : 3 * proj + n + 1] for n in range(3))
                pieces.append((a, b, pltpu.roll(t, 32 * i, 1) if i else t))
            for n, tile in enumerate(joined(pieces, 1)):
                at = pl.ds(128 * (9 * quad + n), 128)
                scales[proj : proj + 1, at] = (tile + EPSILON) / LIMIT
                factor[proj, :, at] = LIMIT / (tile + EPSILON)


def lay_out(blocks, factor, out, p):
    proj = p // PARTS
    rows = pl.ds(pl.multiple_of((p % PARTS) * PART, PART), PART)
    for quad in range(4):
        pieces = []
        for i in range(4):
            value = blocks[4 * quad + i, p].astype(jnp.float32)
            last = value[2 * PART :]
            tail = jnp.concatenate(
                [pltpu.roll(last, (32 * (i - g)) % 128, 1) if i != g else last for g in range(4)],
                axis=0,
            )
            pieces.append((value[:PART], value[PART : 2 * PART], tail))
        for n, tile in enumerate(joined(pieces, PART)):
            at = pl.ds(128 * (9 * quad + n), 128)
            out[proj, rows, at] = (tile * factor[proj, :, at]).astype(jnp.bfloat16)


def move_kernel(
    routes_in, gate, up, final, scales, routes, slab, src, relay, out, packed, line, pieces, peaks, mine, total, gathered, factor,
    slab_sems, sends, relay_sems, out_sems, peak_sems, routes_sem
):
    x, y, z, k = place()
    z_lo, z_hi = z % 2, z // 2
    row, col = lax.axis_index("row"), lax.axis_index("col")
    goal = 2 * z_lo + x // 2
    stay = goal == y
    near = x % 2 == z_hi
    slot = goal * 4 + z_hi * 2 + k
    own = 2 * (z_lo * 4 + x) + k
    keep = jnp.logical_and(near, stay)

    def slab_copy(p, h):
        rows = pl.ds(h * SIDE + p % PARTS * PART, PART)
        return pltpu.make_async_copy(
            (gate, up)[p // PARTS].at[rows], slab.at[2 * p + h], slab_sems.at[2 * p + h]
        )

    routes_copy = pltpu.make_async_copy(routes_in, routes, routes_sem)
    routes_copy.start()
    slab_copy(0, k).start()
    slab_copy(0, 1 - k).start()

    barrier = pltpu.get_barrier_semaphore()
    for n in range(1, 32):
        other = device((x + n // 8) % 4, y, (z + n // 2 % 4) % 4, (k + n % 2) % 2)
        pl.semaphore_signal(barrier, 1, device_id=other, device_id_type=MESH)
    for n in range(12):
        other = device(x, (y + 1 + n // 4) % 4, (z + 2 * (n // 2 % 2)) % 4, (k + n % 2) % 2)
        pl.semaphore_signal(barrier, 1, device_id=other, device_id_type=MESH)

    def first(hi, zi, dx, p):
        h, zl = (k + hi) % 2, (z_lo + zi) % 2
        xd, zd = (x + dx) % 4, 2 * (x % 2) + zl
        block = src.at[2 * (zl * 4 + xd) + h, p]
        to = device(xd, y, zd, h)
        at_all = jnp.logical_not(near) if (hi, zi, dx) == (0, 0, 0) else True

        @pl.when(jnp.logical_and(at_all, stay))
        def _():
            remote(block, out.at[col, p], sends.at[0], out_sems.at[p], to).start()

        @pl.when(jnp.logical_and(at_all, jnp.logical_not(stay)))
        def _():
            remote(block, relay.at[slot, p], sends.at[0], relay_sems.at[slot, p], to).start()

    def second(hi, zi, a, zs, p):
        zl, ks = (z_lo + zi) % 2, (k + hi) % 2
        yd = 2 * zl + a
        q = zs * 2 + ks
        here = yd * 4 + q
        to = device(x, yd, z, k)
        target = out.at[y * 4 + q, p]
        go = yd != y
        if (hi, zi) == (0, 0):
            local = jnp.logical_and(near, jnp.logical_and(yd == goal, zs == z_hi))

            @pl.when(jnp.logical_and(go, local))
            def _():
                remote(src.at[own, p], target, sends.at[1], out_sems.at[p], to).start()

            go = jnp.logical_and(go, jnp.logical_not(local))

        @pl.when(go)
        def _():
            wait_bytes(relay.at[here, p], relay_sems.at[here, p])
            remote(relay.at[here, p], target, sends.at[1], out_sems.at[p], to).start()

    groups = [(0, 0), (0, 1), (1, 0), (1, 1)]
    firsts = [(*g, dx) for g in groups for dx in (1, 3, 2, 0)]
    seconds = [(*g, a, zs) for g in groups for a in range(2) for zs in range(2)]

    def prepare(p, halves=(0, 1)):
        pack(routes, slab, packed, src, p, halves)

    def keep_own(p):
        @pl.when(keep)
        def _():
            out[col, p] = src[own, p]

    def full_round(p, _):
        prepare(p + 2)
        keep_own(p + 2)
        for f, s in zip(firsts, seconds):
            second(*s, p)
            first(*f, p + 2)
        return 0

    def last_round(p, _):
        for s in seconds:
            second(*s, p)
        return 0

    def arrived(p, _):
        @pl.when(keep)
        def _():
            wait_bytes(out.at[pl.ds(0, 15), p], out_sems.at[p])

        @pl.when(jnp.logical_not(keep))
        def _():
            wait_bytes(out.at[:, p], out_sems.at[p])

        lay_out(out, factor, final, p)
        return 0

    for n in range(2, 2 * CHUNKS):
        slab_copy(n // 2, n % 2).start()
    routes_copy.wait()
    slab_copy(0, k).wait()
    prepare(0, (k,))
    pl.semaphore_wait(barrier, 43)
    for f in firsts[:8]:
        first(*f, 0)
    slab_copy(0, 1 - k).wait()
    prepare(0, (1 - k,))
    for f in firsts[8:]:
        first(*f, 0)
    keep_own(0)

    for n in range(2, 2 * CHUNKS):
        slab_copy(n // 2, n % 2).wait()
    local_peaks(routes, slab, line, pieces, peaks)
    mine[row] = peaks[row]
    for n in range(1, 8):
        xd, zl = (x + n % 4) % 4, (z_lo + n // 4) % 2
        to = device(xd, y, 2 * z_hi + zl, k)
        remote(peaks.at[zl * 4 + xd], mine.at[row], sends.at[2], peak_sems.at[0], to).start()

    prepare(1)
    keep_own(1)
    for f in firsts:
        first(*f, 1)
    lax.fori_loop(0, 1, full_round, 0)
    wait_bytes(mine.at[pl.ds(0, 7)], peak_sems.at[0])
    total[...] = jnp.max(mine[...], axis=0)
    gathered[col] = total[...]
    lax.fori_loop(1, 2, full_round, 0)
    for n in range(1, 4):
        to = device(x, y, (z + 2 * (n // 2)) % 4, (k + n % 2) % 2)
        remote(total, gathered.at[col], sends.at[3], peak_sems.at[1], to).start()
    lax.fori_loop(2, 3, full_round, 0)
    lax.fori_loop(3, 4, full_round, 0)
    wait_bytes(gathered.at[pl.ds(0, 3)], peak_sems.at[1])
    four = pl.ds(4 * y, 4)
    for dy in range(1, 4):
        to = device(x, (y + dy) % 4, z, k)
        remote(gathered.at[four], gathered.at[four], sends.at[4], peak_sems.at[2], to).start()
    lax.fori_loop(CHUNKS - 2, CHUNKS - 1, last_round, 0)
    lax.fori_loop(CHUNKS - 1, CHUNKS, last_round, 0)
    wait_bytes(gathered.at[pl.ds(0, 12)], peak_sems.at[2])
    factors(gathered, scales, factor)
    lax.fori_loop(0, CHUNKS, arrived, 0)

    @pl.when(near)
    def _():
        wait_bytes(src.at[pl.ds(0, 15)], sends.at[0])

    @pl.when(jnp.logical_not(near))
    def _():
        wait_bytes(src, sends.at[0])

    wait_bytes(src.at[pl.ds(0, 12)], sends.at[1])
    wait_bytes(mine.at[pl.ds(0, 7)], sends.at[2])
    wait_bytes(gathered.at[pl.ds(0, 3)], sends.at[3])
    wait_bytes(gathered.at[pl.ds(0, 12)], sends.at[4])


def move(gate, up, routes):
    shape = (16, CHUNKS, ROWS, 128)
    return pl.pallas_call(
        move_kernel,
        out_shape=(
            pltpu.VMEM((2, SIDE, 4608), jnp.bfloat16),
            pltpu.VMEM((2, 4608), jnp.float32),
        ),
        in_specs=[
            pl.BlockSpec(memory_space=pltpu.HBM),
            pl.BlockSpec(memory_space=pltpu.HBM),
            pl.BlockSpec(memory_space=pltpu.HBM),
        ],
        out_specs=(pl.BlockSpec(memory_space=pltpu.VMEM),) * 2,
        scratch_shapes=[
            pltpu.SMEM((2, 8), jnp.int32),
            pltpu.VMEM((2 * CHUNKS, PART, 2304), jnp.bfloat16),
            pltpu.VMEM(shape, jnp.bfloat16),
            pltpu.VMEM(shape, jnp.bfloat16),
            pltpu.VMEM(shape, jnp.bfloat16),
            pltpu.VMEM((16, ROWS, 128), jnp.bfloat16),
            pltpu.VMEM((2, 2304), jnp.float32),
            pltpu.VMEM((16, 8, 128), jnp.float32),
            pltpu.VMEM((8, 8, 128), jnp.float32),
            pltpu.VMEM((8, 8, 128), jnp.float32),
            pltpu.VMEM((8, 128), jnp.float32),
            pltpu.VMEM((16, 8, 128), jnp.float32),
            pltpu.VMEM((2, 1, 4608), jnp.float32),
            pltpu.SemaphoreType.DMA((2 * CHUNKS,)),
            pltpu.SemaphoreType.DMA((5,)),
            pltpu.SemaphoreType.DMA((16, CHUNKS)),
            pltpu.SemaphoreType.DMA((CHUNKS,)),
            pltpu.SemaphoreType.DMA((3,)),
            pltpu.SemaphoreType.DMA,
        ],
        compiler_params=pltpu.CompilerParams(
            collective_id=0, has_side_effects=True, vmem_limit_bytes=40 * 2**20
        ),
    )(
        pltpu.with_memory_space_constraint(routes, pltpu.HBM),
        pltpu.with_memory_space_constraint(gate, pltpu.HBM),
        pltpu.with_memory_space_constraint(up, pltpu.HBM),
    )


def store_kernel(final, lines, gate, up, scales, sems):
    copies = [
        pltpu.make_async_copy(
            final.at[proj, pl.ds(i * PART, PART)], ref.at[pl.ds(i * PART, PART)], sems.at[proj * PARTS + i]
        )
        for proj, ref in enumerate((gate, up))
        for i in range(PARTS)
    ]
    copies.append(pltpu.make_async_copy(lines, scales, sems.at[2 * PARTS]))
    for copy in copies:
        copy.start()
    for copy in copies:
        copy.wait()


def store(final, lines):
    return pl.pallas_call(
        store_kernel,
        out_shape=(
            jax.ShapeDtypeStruct((SIDE, 4608), jnp.bfloat16),
            jax.ShapeDtypeStruct((SIDE, 4608), jnp.bfloat16),
            jax.ShapeDtypeStruct((2, 4608), jnp.float32),
        ),
        in_specs=[pl.BlockSpec(memory_space=pltpu.VMEM)] * 2,
        out_specs=(pl.BlockSpec(memory_space=pltpu.HBM),) * 3,
        scratch_shapes=[pltpu.SemaphoreType.DMA((2 * PARTS + 1,))],
        compiler_params=pltpu.CompilerParams(vmem_limit_bytes=2**20),
    )(
        pltpu.with_memory_space_constraint(final, pltpu.VMEM),
        pltpu.with_memory_space_constraint(lines, pltpu.VMEM),
    )


def shards(gate_weight, up_weight, routes):
    return store(*move(gate_weight, up_weight, routes))


def solution(mesh):
    return jax.shard_map(
        shards,
        mesh=mesh,
        in_specs=(P("row", "col"), P("row", "col"), P()),
        out_specs=(P("col", "row"), P("col", "row"), P(None, "row")),
        check_vma=False,
    )
```

```python
import functools

import jax
import jax.numpy as jnp
from jax import lax
from jax.experimental import pallas as pl
from jax.experimental.pallas import tpu as pltpu
from jax.sharding import PartitionSpec as P

MESH = pl.DeviceIdType.MESH
EPSILON = 1e-06
LIMIT = 4.0
SIDE = 288
PART = 96
PARTS = SIDE // PART
TAIL = PART // 4
ROWS = 2 * PART + TAIL
CHUNKS = 2 * PARTS


def lanes(rows):
    return lax.broadcasted_iota(jnp.int32, (rows, 128), 1)


def place():
    r, c = lax.axis_index("row"), lax.axis_index("col")
    return r % 4, c // 4, (c // 2 % 2) * 2 + r // 4, c % 2


def device(x, y, z, k):
    return ((z % 2) * 4 + x, y * 4 + (z // 2) * 2 + k)


def remote(src, dst, send, recv, to):
    return pltpu.make_async_remote_copy(
        src_ref=src, dst_ref=dst, send_sem=send, recv_sem=recv, device_id=to, device_id_type=MESH
    )


def wait_bytes(ref, sem):
    pltpu.make_async_copy(ref, ref, sem).wait()


def aligned(ref, lead, piece):
    start, shift = 9 * piece // 4 * 128, 32 * (piece % 4)
    a, b, c = (
        ref[(*lead, slice(start + 128 * t, start + 128 * (t + 1)))].astype(jnp.float32) for t in range(3)
    )
    if not shift:
        return a, b, c
    a, b, c = (pltpu.roll(value, 128 - shift, 1) for value in (a, b, c))
    keep = lanes(a.shape[0]) < 128 - shift
    return jnp.where(keep, a, b), jnp.where(keep, b, c), c


def pack(routes, slab, packed, src, p, halves):
    lane_tail = lanes(TAIL)
    for piece in range(8):
        for h in halves:
            a, b, c = aligned(slab, (2 * p + h, slice(None)), piece)
            last = c[:TAIL]
            for g in range(1, 4):
                moved = pltpu.roll(c[g * TAIL : (g + 1) * TAIL], 32 * g, 1)
                last = jnp.where(lane_tail < 32 * g, last, moved)
            packed[2 * piece + h, :PART] = a.astype(jnp.bfloat16)
            packed[2 * piece + h, PART : 2 * PART] = b.astype(jnp.bfloat16)
            packed[2 * piece + h, 2 * PART :] = last.astype(jnp.bfloat16)
    for rank in range(8):
        piece = routes[p // PARTS, rank]
        for h in halves:
            src[2 * rank + h, p] = packed[2 * piece + h]


def local_peaks(routes, slab, line, pieces, peaks):
    for proj in range(2):
        for at in range(0, 2304, 256):
            top = jnp.abs(slab[2 * PARTS * proj, :, at : at + 256])
            for n in range(1, 2 * PARTS):
                top = jnp.maximum(top, jnp.abs(slab[2 * PARTS * proj + n, :, at : at + 256]))
            line[proj : proj + 1, at : at + 256] = jnp.max(top.astype(jnp.float32), axis=0, keepdims=True)
    for proj in range(2):
        for piece in range(8):
            rows = aligned(line, (slice(proj, proj + 1),), piece)
            for t in range(3):
                pieces[8 * proj + piece, 3 * proj + t : 3 * proj + t + 1] = rows[t]
    upper = lax.broadcasted_iota(jnp.int32, (8, 128), 0) < 3
    for rank in range(8):
        peaks[rank] = jnp.where(upper, pieces[routes[0, rank]], pieces[8 + routes[1, rank]])


def joined(pieces, rows):
    lane = lanes(rows)
    tiles = []
    spill = None
    for i, (a, b, tail) in enumerate(pieces):
        if i:
            a, b = pltpu.roll(a, 32 * i, 1), pltpu.roll(b, 32 * i, 1)
            tiles.append(jnp.where(lane < 32 * i, spill, a))
            tiles.append(jnp.where(lane < 32 * i, a, b))
            spill = jnp.where(lane < 32 * i, b, tail)
        else:
            tiles += [a, b]
            spill = tail
    tiles.append(spill)
    return tiles


def factors(gathered, scales, factor):
    for proj in range(2):
        for quad in range(4):
            pieces = []
            for i in range(4):
                value = gathered[4 * quad + i]
                a, b, t = (value[3 * proj + n : 3 * proj + n + 1] for n in range(3))
                pieces.append((a, b, pltpu.roll(t, 32 * i, 1) if i else t))
            for n, tile in enumerate(joined(pieces, 1)):
                at = pl.ds(128 * (9 * quad + n), 128)
                scales[proj : proj + 1, at] = (tile + EPSILON) / LIMIT
                factor[proj, :, at] = LIMIT / (tile + EPSILON)


def lay_out(blocks, factor, out, p):
    proj = p // PARTS
    rows = pl.ds(p % PARTS * PART, PART) if isinstance(p, int) else pl.ds(pl.multiple_of(p % PARTS * PART, PART), PART)
    for quad in range(4):
        pieces = []
        for i in range(4):
            value = blocks[4 * quad + i, p].astype(jnp.float32)
            last = value[2 * PART :]
            tail = jnp.concatenate(
                [pltpu.roll(last, (32 * (i - g)) % 128, 1) if i != g else last for g in range(4)],
                axis=0,
            )
            pieces.append((value[:PART], value[PART : 2 * PART], tail))
        for n, tile in enumerate(joined(pieces, PART)):
            at = pl.ds(128 * (9 * quad + n), 128)
            out[proj, rows, at] = (tile * factor[proj, :, at]).astype(jnp.bfloat16)


def move_kernel(
    routes_in, gate, up, final, out, scales, factor, routes, slab, src, relay, packed, line, pieces, peaks, mine, total, gathered,
    slab_sems, sends, relay_sems, out_sems, peak_sems, routes_sem
):
    x, y, z, k = place()
    z_lo, z_hi = z % 2, z // 2
    row, col = lax.axis_index("row"), lax.axis_index("col")
    goal = 2 * z_lo + x // 2
    stay = goal == y
    near = x % 2 == z_hi
    slot = goal * 4 + z_hi * 2 + k
    own = 2 * (z_lo * 4 + x) + k
    keep = jnp.logical_and(near, stay)

    def slab_copy(p, h):
        rows = pl.ds(h * SIDE + p % PARTS * PART, PART)
        return pltpu.make_async_copy(
            (gate, up)[p // PARTS].at[rows], slab.at[2 * p + h], slab_sems.at[2 * p + h]
        )

    routes_copy = pltpu.make_async_copy(routes_in, routes, routes_sem)
    routes_copy.start()
    slab_copy(0, k).start()
    slab_copy(0, 1 - k).start()

    barrier = pltpu.get_barrier_semaphore()
    for n in range(1, 32):
        other = device((x + n // 8) % 4, y, (z + n // 2 % 4) % 4, (k + n % 2) % 2)
        pl.semaphore_signal(barrier, 1, device_id=other, device_id_type=MESH)
    for n in range(12):
        other = device(x, (y + 1 + n // 4) % 4, (z + 2 * (n // 2 % 2)) % 4, (k + n % 2) % 2)
        pl.semaphore_signal(barrier, 1, device_id=other, device_id_type=MESH)

    def first(hi, zi, dx, p):
        h, zl = (k + hi) % 2, (z_lo + z_hi + zi) % 2
        xd, zd = (x + dx) % 4, 2 * (x % 2) + zl
        block = src.at[2 * (zl * 4 + xd) + h, p]
        to = device(xd, y, zd, h)
        at_all = jnp.logical_not(jnp.logical_and(near, zl == z_lo)) if (hi, dx) == (0, 0) else True

        @pl.when(jnp.logical_and(at_all, stay))
        def _():
            remote(block, out.at[col, p], sends.at[0], out_sems.at[p], to).start()

        @pl.when(jnp.logical_and(at_all, jnp.logical_not(stay)))
        def _():
            remote(block, relay.at[slot, p], sends.at[0], relay_sems.at[slot, p], to).start()

    def second(hi, zi, a, zl, p):
        zs, ks = (z_lo + zi + zl) % 2, (k + hi) % 2
        yd = 2 * zl + a
        q = zs * 2 + ks
        here = yd * 4 + q
        to = device(x, yd, z, k)
        target = out.at[y * 4 + q, p]
        go = yd != y
        if hi == 0:
            local = jnp.logical_and(near, jnp.logical_and(yd == goal, zs == z_hi))

            @pl.when(jnp.logical_and(go, local))
            def _():
                remote(src.at[own, p], target, sends.at[1], out_sems.at[p], to).start()

            go = jnp.logical_and(go, jnp.logical_not(local))

        @pl.when(go)
        def _():
            wait_bytes(relay.at[here, p], relay_sems.at[here, p])
            remote(relay.at[here, p], target, sends.at[1], out_sems.at[p], to).start()

    groups = [(0, 0), (0, 1), (1, 0), (1, 1)]
    firsts = [(*g, dx) for g in groups for dx in (1, 3, 2, 0)]
    seconds = [(*g, a, zl) for g in groups for zl in range(2) for a in range(2)]

    def prepare(p, halves=(0, 1)):
        pack(routes, slab, packed, src, p, halves)

    def keep_own(p):
        @pl.when(keep)
        def _():
            out[col, p] = src[own, p]

    def full_round(p, _):
        prepare(p + 2)
        keep_own(p + 2)
        for f, s in zip(firsts, seconds):
            second(*s, p)
            first(*f, p + 2)
        return 0

    def last_round(p, _):
        for s in seconds:
            second(*s, p)
        return 0

    def arrived(p, _):
        @pl.when(keep)
        def _():
            wait_bytes(out.at[pl.ds(0, 15), p], out_sems.at[p])

        @pl.when(jnp.logical_not(keep))
        def _():
            wait_bytes(out.at[:, p], out_sems.at[p])

        @pl.when(p < CHUNKS - 1)
        def _():
            lay_out(out, factor, final, p)

        return 0

    for n in range(2, 2 * CHUNKS):
        slab_copy(n // 2, n % 2).start()
    routes_copy.wait()
    slab_copy(0, k).wait()
    prepare(0, (k,))
    pl.semaphore_wait(barrier, 43)
    for f in firsts[:8]:
        first(*f, 0)
    slab_copy(0, 1 - k).wait()
    prepare(0, (1 - k,))
    for f in firsts[8:]:
        first(*f, 0)
    keep_own(0)

    for n in range(2, 2 * CHUNKS):
        slab_copy(n // 2, n % 2).wait()
    local_peaks(routes, slab, line, pieces, peaks)
    mine[row] = peaks[row]
    for n in range(1, 8):
        xd, zl = (x + n % 4) % 4, (z_lo + n // 4) % 2
        to = device(xd, y, 2 * z_hi + zl, k)
        remote(peaks.at[zl * 4 + xd], mine.at[row], sends.at[2], peak_sems.at[0], to).start()

    prepare(1)
    keep_own(1)
    for f in firsts:
        first(*f, 1)
    lax.fori_loop(0, 1, full_round, 0)
    wait_bytes(mine.at[pl.ds(0, 7)], peak_sems.at[0])
    total[...] = jnp.max(mine[...], axis=0)
    gathered[col] = total[...]
    lax.fori_loop(1, 2, full_round, 0)
    for n in range(1, 4):
        to = device(x, y, (z + 2 * (n // 2)) % 4, (k + n % 2) % 2)
        remote(total, gathered.at[col], sends.at[3], peak_sems.at[1], to).start()
    lax.fori_loop(2, 3, full_round, 0)
    lax.fori_loop(3, 4, full_round, 0)
    wait_bytes(gathered.at[pl.ds(0, 3)], peak_sems.at[1])
    four = pl.ds(4 * y, 4)
    for dy in range(1, 4):
        to = device(x, (y + dy) % 4, z, k)
        remote(gathered.at[four], gathered.at[four], sends.at[4], peak_sems.at[2], to).start()
    lax.fori_loop(CHUNKS - 2, CHUNKS - 1, last_round, 0)
    lax.fori_loop(CHUNKS - 1, CHUNKS, last_round, 0)
    wait_bytes(gathered.at[pl.ds(0, 12)], peak_sems.at[2])
    factors(gathered, scales, factor)
    lax.fori_loop(0, CHUNKS, arrived, 0)

    @pl.when(near)
    def _():
        wait_bytes(src.at[pl.ds(0, 15)], sends.at[0])

    @pl.when(jnp.logical_not(near))
    def _():
        wait_bytes(src, sends.at[0])

    wait_bytes(src.at[pl.ds(0, 12)], sends.at[1])
    wait_bytes(mine.at[pl.ds(0, 7)], sends.at[2])
    wait_bytes(gathered.at[pl.ds(0, 3)], sends.at[3])
    wait_bytes(gathered.at[pl.ds(0, 12)], sends.at[4])


def move(gate, up, routes):
    shape = (16, CHUNKS, ROWS, 128)
    return pl.pallas_call(
        move_kernel,
        out_shape=(
            pltpu.VMEM((2, SIDE, 4608), jnp.bfloat16),
            pltpu.VMEM(shape, jnp.bfloat16),
            pltpu.VMEM((2, 4608), jnp.float32),
            pltpu.VMEM((2, 1, 4608), jnp.float32),
        ),
        in_specs=[
            pl.BlockSpec(memory_space=pltpu.HBM),
            pl.BlockSpec(memory_space=pltpu.HBM),
            pl.BlockSpec(memory_space=pltpu.HBM),
        ],
        out_specs=(pl.BlockSpec(memory_space=pltpu.VMEM),) * 4,
        scratch_shapes=[
            pltpu.SMEM((2, 8), jnp.int32),
            pltpu.VMEM((2 * CHUNKS, PART, 2304), jnp.bfloat16),
            pltpu.VMEM(shape, jnp.bfloat16),
            pltpu.VMEM(shape, jnp.bfloat16),
            pltpu.VMEM((16, ROWS, 128), jnp.bfloat16),
            pltpu.VMEM((2, 2304), jnp.float32),
            pltpu.VMEM((16, 8, 128), jnp.float32),
            pltpu.VMEM((8, 8, 128), jnp.float32),
            pltpu.VMEM((8, 8, 128), jnp.float32),
            pltpu.VMEM((8, 128), jnp.float32),
            pltpu.VMEM((16, 8, 128), jnp.float32),
            pltpu.SemaphoreType.DMA((2 * CHUNKS,)),
            pltpu.SemaphoreType.DMA((5,)),
            pltpu.SemaphoreType.DMA((16, CHUNKS)),
            pltpu.SemaphoreType.DMA((CHUNKS,)),
            pltpu.SemaphoreType.DMA((3,)),
            pltpu.SemaphoreType.DMA,
        ],
        compiler_params=pltpu.CompilerParams(
            collective_id=0, has_side_effects=True, vmem_limit_bytes=40 * 2**20
        ),
    )(
        pltpu.with_memory_space_constraint(routes, pltpu.HBM),
        pltpu.with_memory_space_constraint(gate, pltpu.HBM),
        pltpu.with_memory_space_constraint(up, pltpu.HBM),
    )


def store_kernel(final, blocks, lines, factor, gate, up, scales, last, sems):
    copies = [
        pltpu.make_async_copy(
            (last if n == CHUNKS - 1 else final).at[n // PARTS, pl.ds(n % PARTS * PART, PART)],
            (gate, up)[n // PARTS].at[pl.ds(n % PARTS * PART, PART)],
            sems.at[n],
        )
        for n in range(CHUNKS)
    ]
    copies.insert(CHUNKS - 1, pltpu.make_async_copy(lines, scales, sems.at[CHUNKS]))
    for copy in copies[:-1]:
        copy.start()
    lay_out(blocks, factor, last, CHUNKS - 1)
    copies[-1].start()
    for copy in copies:
        copy.wait()


def store(*results):
    return pl.pallas_call(
        store_kernel,
        out_shape=(
            jax.ShapeDtypeStruct((SIDE, 4608), jnp.bfloat16),
            jax.ShapeDtypeStruct((SIDE, 4608), jnp.bfloat16),
            jax.ShapeDtypeStruct((2, 4608), jnp.float32),
        ),
        in_specs=[pl.BlockSpec(memory_space=pltpu.VMEM)] * 4,
        out_specs=(pl.BlockSpec(memory_space=pltpu.HBM),) * 3,
        scratch_shapes=[
            pltpu.VMEM((2, SIDE, 4608), jnp.bfloat16),
            pltpu.SemaphoreType.DMA((CHUNKS + 1,)),
        ],
        compiler_params=pltpu.CompilerParams(vmem_limit_bytes=10 * 2**20),
    )(*(pltpu.with_memory_space_constraint(result, pltpu.VMEM) for result in results))


def shards(gate_weight, up_weight, routes):
    return store(*move(gate_weight, up_weight, routes))


def solution(mesh):
    return jax.shard_map(
        shards,
        mesh=mesh,
        in_specs=(P("row", "col"), P("row", "col"), P()),
        out_specs=(P("col", "row"), P("col", "row"), P(None, "row")),
        check_vma=False,
    )
```

```python
import functools

import jax
import jax.numpy as jnp
from jax import lax
from jax.experimental import pallas as pl
from jax.experimental.pallas import tpu as pltpu
from jax.sharding import PartitionSpec as P

MESH = pl.DeviceIdType.MESH
EPSILON = 1e-06
LIMIT = 4.0
SIDE = 288
PART = 96
PARTS = SIDE // PART
TAIL = PART // 4
ROWS = 2 * PART + TAIL
CHUNKS = 2 * PARTS


def lanes(rows):
    return lax.broadcasted_iota(jnp.int32, (rows, 128), 1)


def place():
    r, c = lax.axis_index("row"), lax.axis_index("col")
    return r % 4, c // 4, (c // 2 % 2) * 2 + r // 4, c % 2


def device(x, y, z, k):
    return ((z % 2) * 4 + x, y * 4 + (z // 2) * 2 + k)


def remote(src, dst, send, recv, to):
    return pltpu.make_async_remote_copy(
        src_ref=src, dst_ref=dst, send_sem=send, recv_sem=recv, device_id=to, device_id_type=MESH
    )


def wait_bytes(ref, sem):
    pltpu.make_async_copy(ref, ref, sem).wait()


def aligned(ref, lead, piece):
    start, shift = 9 * piece // 4 * 128, 32 * (piece % 4)
    a, b, c = (
        ref[(*lead, slice(start + 128 * t, start + 128 * (t + 1)))].astype(jnp.float32) for t in range(3)
    )
    if not shift:
        return a, b, c
    a, b, c = (pltpu.roll(value, 128 - shift, 1) for value in (a, b, c))
    keep = lanes(a.shape[0]) < 128 - shift
    return jnp.where(keep, a, b), jnp.where(keep, b, c), c


def pack(routes, slab, packed, src, p, halves):
    lane_tail = lanes(TAIL)
    for piece in range(8):
        for h in halves:
            a, b, c = aligned(slab, (2 * p + h, slice(None)), piece)
            last = c[:TAIL]
            for g in range(1, 4):
                moved = pltpu.roll(c[g * TAIL : (g + 1) * TAIL], 32 * g, 1)
                last = jnp.where(lane_tail < 32 * g, last, moved)
            packed[2 * piece + h, :PART] = a.astype(jnp.bfloat16)
            packed[2 * piece + h, PART : 2 * PART] = b.astype(jnp.bfloat16)
            packed[2 * piece + h, 2 * PART :] = last.astype(jnp.bfloat16)
    for rank in range(8):
        piece = routes[p // PARTS, rank]
        for h in halves:
            src[2 * rank + h, p] = packed[2 * piece + h]


def local_peaks(routes, slab, line, pieces, peaks):
    for proj in range(2):
        for at in range(0, 2304, 256):
            top = jnp.abs(slab[2 * PARTS * proj, :, at : at + 256])
            for n in range(1, 2 * PARTS):
                top = jnp.maximum(top, jnp.abs(slab[2 * PARTS * proj + n, :, at : at + 256]))
            line[proj : proj + 1, at : at + 256] = jnp.max(top.astype(jnp.float32), axis=0, keepdims=True)
    for proj in range(2):
        for piece in range(8):
            rows = aligned(line, (slice(proj, proj + 1),), piece)
            for t in range(3):
                pieces[8 * proj + piece, 3 * proj + t : 3 * proj + t + 1] = rows[t]
    upper = lax.broadcasted_iota(jnp.int32, (8, 128), 0) < 3
    for rank in range(8):
        peaks[rank] = jnp.where(upper, pieces[routes[0, rank]], pieces[8 + routes[1, rank]])


def joined(pieces, rows):
    lane = lanes(rows)
    tiles = []
    spill = None
    for i, (a, b, tail) in enumerate(pieces):
        if i:
            a, b = pltpu.roll(a, 32 * i, 1), pltpu.roll(b, 32 * i, 1)
            tiles.append(jnp.where(lane < 32 * i, spill, a))
            tiles.append(jnp.where(lane < 32 * i, a, b))
            spill = jnp.where(lane < 32 * i, b, tail)
        else:
            tiles += [a, b]
            spill = tail
    tiles.append(spill)
    return tiles


def factors(gathered, scales, factor):
    for proj in range(2):
        for quad in range(4):
            pieces = []
            for i in range(4):
                value = gathered[4 * quad + i]
                a, b, t = (value[3 * proj + n : 3 * proj + n + 1] for n in range(3))
                pieces.append((a, b, pltpu.roll(t, 32 * i, 1) if i else t))
            for n, tile in enumerate(joined(pieces, 1)):
                at = pl.ds(128 * (9 * quad + n), 128)
                scales[proj : proj + 1, at] = (tile + EPSILON) / LIMIT
                factor[proj, :, at] = LIMIT / (tile + EPSILON)


def lay_out(blocks, factor, out, p):
    proj = p // PARTS
    rows = pl.ds(p % PARTS * PART, PART) if isinstance(p, int) else pl.ds(pl.multiple_of(p % PARTS * PART, PART), PART)
    for quad in range(4):
        pieces = []
        for i in range(4):
            value = blocks[4 * quad + i, p].astype(jnp.float32)
            last = value[2 * PART :]
            tail = jnp.concatenate(
                [pltpu.roll(last, (32 * (i - g)) % 128, 1) if i != g else last for g in range(4)],
                axis=0,
            )
            pieces.append((value[:PART], value[PART : 2 * PART], tail))
        for n, tile in enumerate(joined(pieces, PART)):
            at = pl.ds(128 * (9 * quad + n), 128)
            out[proj, rows, at] = (tile * factor[proj, :, at]).astype(jnp.bfloat16)


def move_kernel(
    routes_in, gate, up, final, out, scales, factor, routes, slab, src, relay, packed, line, pieces, peaks, mine, total, gathered,
    slab_sems, sends, relay_sems, out_sems, peak_sems, routes_sem
):
    x, y, z, k = place()
    z_lo, z_hi = z % 2, z // 2
    row, col = lax.axis_index("row"), lax.axis_index("col")
    goal = 2 * z_lo + x // 2
    stay = goal == y
    near = x % 2 == z_hi
    slot = goal * 4 + z_hi * 2 + k
    own = 2 * (z_lo * 4 + x) + k
    keep = jnp.logical_and(near, stay)

    def slab_copy(p, h):
        rows = pl.ds(h * SIDE + p % PARTS * PART, PART)
        return pltpu.make_async_copy(
            (gate, up)[p // PARTS].at[rows], slab.at[2 * p + h], slab_sems.at[2 * p + h]
        )

    routes_copy = pltpu.make_async_copy(routes_in, routes, routes_sem)
    routes_copy.start()
    slab_copy(0, k).start()
    slab_copy(0, 1 - k).start()

    barrier = pltpu.get_barrier_semaphore()
    for n in range(1, 32):
        other = device((x + n // 8) % 4, y, (z + n // 2 % 4) % 4, (k + n % 2) % 2)
        pl.semaphore_signal(barrier, 1, device_id=other, device_id_type=MESH)
    for n in range(12):
        other = device(x, (y + 1 + n // 4) % 4, (z + 2 * (n // 2 % 2)) % 4, (k + n % 2) % 2)
        pl.semaphore_signal(barrier, 1, device_id=other, device_id_type=MESH)

    def first(hi, zi, dx, p):
        h, zl = (k + hi) % 2, (z_lo + z_hi + zi) % 2
        xd, zd = (x + dx) % 4, 2 * (x % 2) + zl
        block = src.at[2 * (zl * 4 + xd) + h, p]
        to = device(xd, y, zd, h)
        at_all = jnp.logical_not(jnp.logical_and(near, zl == z_lo)) if (hi, dx) == (0, 0) else True

        @pl.when(jnp.logical_and(at_all, stay))
        def _():
            remote(block, out.at[col, p], sends.at[0], out_sems.at[p], to).start()

        @pl.when(jnp.logical_and(at_all, jnp.logical_not(stay)))
        def _():
            remote(block, relay.at[slot, p], sends.at[0], relay_sems.at[slot, p], to).start()

    def second(hi, zi, a, zl, p):
        zs, ks = (z_lo + zi + zl) % 2, (k + hi) % 2
        yd = 2 * zl + a
        q = zs * 2 + ks
        here = yd * 4 + q
        to = device(x, yd, z, k)
        target = out.at[y * 4 + q, p]
        go = yd != y
        if hi == 0:
            local = jnp.logical_and(near, jnp.logical_and(yd == goal, zs == z_hi))

            @pl.when(jnp.logical_and(go, local))
            def _():
                remote(src.at[own, p], target, sends.at[1], out_sems.at[p], to).start()

            go = jnp.logical_and(go, jnp.logical_not(local))

        @pl.when(go)
        def _():
            wait_bytes(relay.at[here, p], relay_sems.at[here, p])
            remote(relay.at[here, p], target, sends.at[1], out_sems.at[p], to).start()

    groups = [(0, 0), (0, 1), (1, 0), (1, 1)]
    firsts = [(*g, dx) for g in groups for dx in (1, 3, 2, 0)]
    seconds = [(*g, a, zl) for g in groups for zl in range(2) for a in range(2)]

    def prepare(p, halves=(0, 1)):
        pack(routes, slab, packed, src, p, halves)

    def keep_own(p):
        @pl.when(keep)
        def _():
            out[col, p] = src[own, p]

    def full_round(p, _):
        prepare(p + 2)
        keep_own(p + 2)
        for f, s in zip(firsts, seconds):
            second(*s, p)
            first(*f, p + 2)
        return 0

    def last_round(p, _):
        for s in seconds:
            second(*s, p)
        return 0

    def arrived(p, _):
        @pl.when(keep)
        def _():
            wait_bytes(out.at[pl.ds(0, 15), p], out_sems.at[p])

        @pl.when(jnp.logical_not(keep))
        def _():
            wait_bytes(out.at[:, p], out_sems.at[p])

        @pl.when(p < CHUNKS - 1)
        def _():
            lay_out(out, factor, final, p)

        return 0

    for n in range(2, 2 * CHUNKS):
        slab_copy(n // 2, n % 2).start()
    routes_copy.wait()
    slab_copy(0, k).wait()
    prepare(0, (k,))
    pl.semaphore_wait(barrier, 43)
    for f in firsts[:8]:
        first(*f, 0)
    slab_copy(0, 1 - k).wait()
    prepare(0, (1 - k,))
    for f in firsts[8:]:
        first(*f, 0)
    keep_own(0)

    for n in range(2, 2 * CHUNKS):
        slab_copy(n // 2, n % 2).wait()
    local_peaks(routes, slab, line, pieces, peaks)
    mine[row] = peaks[row]
    for n in range(1, 8):
        xd, zl = (x + n % 4) % 4, (z_lo + n // 4) % 2
        to = device(xd, y, 2 * z_hi + zl, k)
        remote(peaks.at[zl * 4 + xd], mine.at[row], sends.at[2], peak_sems.at[0], to).start()

    prepare(1)
    keep_own(1)
    for f in firsts:
        first(*f, 1)
    lax.fori_loop(0, 1, full_round, 0)
    wait_bytes(mine.at[pl.ds(0, 7)], peak_sems.at[0])
    total[...] = jnp.max(mine[...], axis=0)
    gathered[col] = total[...]
    for n in range(1, 4):
        to = device(x, y, (z + 2 * (n // 2)) % 4, (k + n % 2) % 2)
        remote(total, gathered.at[col], sends.at[3], peak_sems.at[1], to).start()
    lax.fori_loop(1, 2, full_round, 0)
    lax.fori_loop(2, 3, full_round, 0)
    lax.fori_loop(3, 4, full_round, 0)
    wait_bytes(gathered.at[pl.ds(0, 3)], peak_sems.at[1])
    four = pl.ds(4 * y, 4)
    for dy in range(1, 4):
        to = device(x, (y + dy) % 4, z, k)
        remote(gathered.at[four], gathered.at[four], sends.at[4], peak_sems.at[2], to).start()
    lax.fori_loop(CHUNKS - 2, CHUNKS - 1, last_round, 0)
    lax.fori_loop(CHUNKS - 1, CHUNKS, last_round, 0)
    wait_bytes(gathered.at[pl.ds(0, 12)], peak_sems.at[2])
    factors(gathered, scales, factor)
    lax.fori_loop(0, CHUNKS, arrived, 0)

    @pl.when(near)
    def _():
        wait_bytes(src.at[pl.ds(0, 15)], sends.at[0])

    @pl.when(jnp.logical_not(near))
    def _():
        wait_bytes(src, sends.at[0])

    wait_bytes(src.at[pl.ds(0, 12)], sends.at[1])
    wait_bytes(mine.at[pl.ds(0, 7)], sends.at[2])
    wait_bytes(gathered.at[pl.ds(0, 3)], sends.at[3])
    wait_bytes(gathered.at[pl.ds(0, 12)], sends.at[4])


def move(gate, up, routes):
    shape = (16, CHUNKS, ROWS, 128)
    return pl.pallas_call(
        move_kernel,
        out_shape=(
            pltpu.VMEM((2, SIDE, 4608), jnp.bfloat16),
            pltpu.VMEM(shape, jnp.bfloat16),
            pltpu.VMEM((2, 4608), jnp.float32),
            pltpu.VMEM((2, 1, 4608), jnp.float32),
        ),
        in_specs=[
            pl.BlockSpec(memory_space=pltpu.HBM),
            pl.BlockSpec(memory_space=pltpu.HBM),
            pl.BlockSpec(memory_space=pltpu.HBM),
        ],
        out_specs=(pl.BlockSpec(memory_space=pltpu.VMEM),) * 4,
        scratch_shapes=[
            pltpu.SMEM((2, 8), jnp.int32),
            pltpu.VMEM((2 * CHUNKS, PART, 2304), jnp.bfloat16),
            pltpu.VMEM(shape, jnp.bfloat16),
            pltpu.VMEM(shape, jnp.bfloat16),
            pltpu.VMEM((16, ROWS, 128), jnp.bfloat16),
            pltpu.VMEM((2, 2304), jnp.float32),
            pltpu.VMEM((16, 8, 128), jnp.float32),
            pltpu.VMEM((8, 8, 128), jnp.float32),
            pltpu.VMEM((8, 8, 128), jnp.float32),
            pltpu.VMEM((8, 128), jnp.float32),
            pltpu.VMEM((16, 8, 128), jnp.float32),
            pltpu.SemaphoreType.DMA((2 * CHUNKS,)),
            pltpu.SemaphoreType.DMA((5,)),
            pltpu.SemaphoreType.DMA((16, CHUNKS)),
            pltpu.SemaphoreType.DMA((CHUNKS,)),
            pltpu.SemaphoreType.DMA((3,)),
            pltpu.SemaphoreType.DMA,
        ],
        compiler_params=pltpu.CompilerParams(
            collective_id=0, has_side_effects=True, vmem_limit_bytes=40 * 2**20
        ),
    )(
        pltpu.with_memory_space_constraint(routes, pltpu.HBM),
        pltpu.with_memory_space_constraint(gate, pltpu.HBM),
        pltpu.with_memory_space_constraint(up, pltpu.HBM),
    )


def store_kernel(final, blocks, lines, factor, gate, up, scales, last, sems):
    copies = [
        pltpu.make_async_copy(
            (last if n == CHUNKS - 1 else final).at[n // PARTS, pl.ds(n % PARTS * PART, PART)],
            (gate, up)[n // PARTS].at[pl.ds(n % PARTS * PART, PART)],
            sems.at[n],
        )
        for n in range(CHUNKS)
    ]
    copies.insert(CHUNKS - 1, pltpu.make_async_copy(lines, scales, sems.at[CHUNKS]))
    for copy in copies[:-1]:
        copy.start()
    lay_out(blocks, factor, last, CHUNKS - 1)
    copies[-1].start()
    for copy in copies:
        copy.wait()


def store(*results):
    return pl.pallas_call(
        store_kernel,
        out_shape=(
            jax.ShapeDtypeStruct((SIDE, 4608), jnp.bfloat16),
            jax.ShapeDtypeStruct((SIDE, 4608), jnp.bfloat16),
            jax.ShapeDtypeStruct((2, 4608), jnp.float32),
        ),
        in_specs=[pl.BlockSpec(memory_space=pltpu.VMEM)] * 4,
        out_specs=(pl.BlockSpec(memory_space=pltpu.HBM),) * 3,
        scratch_shapes=[
            pltpu.VMEM((2, SIDE, 4608), jnp.bfloat16),
            pltpu.SemaphoreType.DMA((CHUNKS + 1,)),
        ],
        compiler_params=pltpu.CompilerParams(vmem_limit_bytes=10 * 2**20),
    )(*(pltpu.with_memory_space_constraint(result, pltpu.VMEM) for result in results))


def shards(gate_weight, up_weight, routes):
    return store(*move(gate_weight, up_weight, routes))


def solution(mesh):
    return jax.shard_map(
        shards,
        mesh=mesh,
        in_specs=(P("row", "col"), P("row", "col"), P()),
        out_specs=(P("col", "row"), P("col", "row"), P(None, "row")),
        check_vma=False,
    )
```
